128 devices in a mesh: replica: 1, data: 128 (over z, y, x, core).
Axes of the slice: x: 4, y: 4, z: 4, core: 2. Of those that a mesh axis runs over, the one named last changes fastest.
Arguments:
- query_hidden: bfloat16 [1024, 32, 768], P(('replica', 'data'))
- doc_hidden: bfloat16 [1024, 300, 768], P(('replica', 'data'))
- neg_hidden: bfloat16 [1024, 2, 300, 768], P(('replica', 'data'))
- query_mask: int32 [1024, 32], P(('replica', 'data'))
- doc_mask: int32 [1024, 300], P(('replica', 'data'))
- neg_mask: int32 [1024, 2, 300], P(('replica', 'data'))
- teacher: float32 [1024, 3], P(('replica', 'data'))
- w_proj: bfloat16 [768, 128], replicated
- temperature: float32 [], replicated
Outputs:
- output 1: float32 [1024], P(('replica', 'data'))
- output 2: float32 [1], P('replica')
All inputs are finite; a program needn't handle non-finite values.
Results may differ from the reference program's by a relative error of at most 0.001.
Values are sent between devices in bfloat16 or wider.
A program may use at most 1 GiB of HBM per device.

```python
import jax
import jax.numpy as jnp
from jax import lax

BATCH = 1024
QUERY_LEN = 32
DOC_LEN = 300
HIDDEN = 768
PROJ_DIM = 128
NUM_HARD = 2


def project_tokens(hidden, w_proj):
    flat_hidden = hidden.reshape(-1, HIDDEN)
    projected = jnp.dot(flat_hidden, w_proj, preferred_element_type=jnp.float32)
    projected = projected / jnp.sqrt(jnp.sum(projected * projected, axis=-1, keepdims=True))
    return projected.astype(jnp.bfloat16).reshape(hidden.shape[:-1] + (PROJ_DIM,))


def prefix_mask(lengths, width):
    return (jnp.arange(width) < lengths[..., None]).astype(jnp.int32)


def setup_inputs(seed: int = 0, part: int = 0) -> dict:
    root_key = jax.random.key(seed)
    key_w, key_temp, key_common, key_part = jax.random.split(root_key, 4)
    part_keys = jax.random.split(jax.random.fold_in(key_part, part), 10)
    common = jax.random.normal(key_common, (HIDDEN,), jnp.float32)
    base_vec = 0.59 * common
    pair_vec = jax.random.normal(part_keys[0], (BATCH, HIDDEN), jnp.float32)
    query_noise = jax.random.normal(part_keys[1], (BATCH, QUERY_LEN, HIDDEN), jnp.float32)
    query_real = base_vec + 0.39 * pair_vec[:, None, :] + 0.71 * query_noise
    copies = -(-DOC_LEN // QUERY_LEN)
    query_tiled = 2.0 * jnp.tile(query_real, (1, copies, 1))[:, :DOC_LEN]
    query_len = jax.random.randint(part_keys[2], (BATCH,), QUERY_LEN // 2, QUERY_LEN + 1, dtype=jnp.int32).at[0].set(QUERY_LEN)
    doc_len = jax.random.randint(part_keys[3], (BATCH,), DOC_LEN // 4, DOC_LEN + 1, dtype=jnp.int32).at[0].set(DOC_LEN)
    neg_len = jax.random.randint(part_keys[4], (BATCH, NUM_HARD), DOC_LEN // 4, DOC_LEN + 1, dtype=jnp.int32).at[0, 0].set(DOC_LEN)
    query_mask = prefix_mask(query_len, QUERY_LEN)
    doc_mask = prefix_mask(doc_len, DOC_LEN)
    neg_mask = prefix_mask(neg_len, DOC_LEN)
    doc_noise = jax.random.normal(part_keys[5], (BATCH, DOC_LEN, HIDDEN), jnp.float32)
    doc_real = base_vec + 0.39 * pair_vec[:, None, :] + 0.71 * doc_noise
    doc_hidden = jnp.where(doc_mask[:, :, None] > 0, doc_real, query_tiled + 0.3 * doc_noise)
    neg_share = jax.random.uniform(part_keys[6], (BATCH, NUM_HARD, 1, 1), jnp.float32, minval=0.4, maxval=0.9)
    neg_vec = jax.random.normal(part_keys[7], (BATCH, NUM_HARD, 1, HIDDEN), jnp.float32)
    neg_mix = neg_share * pair_vec[:, None, None, :] + jnp.sqrt(1.0 - neg_share * neg_share) * neg_vec
    neg_noise = jax.random.normal(part_keys[8], (BATCH, NUM_HARD, DOC_LEN, HIDDEN), jnp.float32)
    neg_real = base_vec + 0.39 * neg_mix + 0.71 * neg_noise
    neg_hidden = jnp.where(neg_mask[..., None] > 0, neg_real, query_tiled[:, None] + 0.3 * neg_noise)
    teacher = jax.random.normal(part_keys[9], (BATCH, NUM_HARD + 1), jnp.float32).at[:, 0].add(2.0)
    w_proj = jax.random.normal(key_w, (HIDDEN, PROJ_DIM), jnp.float32) * HIDDEN ** -0.5
    temperature = QUERY_LEN * jax.random.uniform(key_temp, (), jnp.float32, minval=0.04, maxval=0.07)
    return {
        'query_hidden': query_real.astype(jnp.bfloat16),
        'doc_hidden': doc_hidden.astype(jnp.bfloat16),
        'neg_hidden': neg_hidden.astype(jnp.bfloat16),
        'query_mask': query_mask,
        'doc_mask': doc_mask,
        'neg_mask': neg_mask,
        'teacher': teacher,
        'w_proj': w_proj.astype(jnp.bfloat16),
        'temperature': temperature,
    }


def reference(query_hidden, doc_hidden, neg_hidden, query_mask, doc_mask, neg_mask, teacher, w_proj, temperature):
    query_tok = project_tokens(query_hidden, w_proj).astype(jnp.float32)
    doc_tok = project_tokens(doc_hidden, w_proj).astype(jnp.float32)
    neg_tok = project_tokens(neg_hidden, w_proj).astype(jnp.float32)
    query_weight = query_mask.astype(jnp.float32)
    doc_valid = doc_mask > 0

    def score_query(query_item):
        query_rows, row_weight, neg_rows, neg_valid = query_item
        sim_tile = jnp.einsum('td,jsd->tjs', query_rows, doc_tok)
        best_sim = jnp.max(jnp.where(doc_valid[None], sim_tile, -jnp.inf), axis=2)
        in_batch = jnp.sum(row_weight[:, None] * best_sim, axis=0)
        hard_sim = jnp.einsum('td,ksd->tks', query_rows, neg_rows)
        hard_best = jnp.max(jnp.where(neg_valid[None] > 0, hard_sim, -jnp.inf), axis=2)
        hard_row = jnp.sum(row_weight[:, None] * hard_best, axis=0)
        return in_batch, hard_row

    scores, hard_scores = lax.map(score_query, (query_tok, query_weight, neg_tok, neg_mask))
    logits = scores / temperature
    positive = jnp.diagonal(logits)
    cross_ent = jax.nn.logsumexp(logits, axis=1) - positive
    student = jnp.concatenate([positive[:, None], hard_scores / temperature], axis=1)
    student_log = jax.nn.log_softmax(student, axis=1)
    teacher_log = jax.nn.log_softmax(teacher, axis=1)
    kl_div = jnp.sum(jnp.exp(teacher_log) * (teacher_log - student_log), axis=1)
    loss_rows = cross_ent + kl_div
    return loss_rows, jnp.mean(loss_rows, keepdims=True)
```

```python
import functools

import jax
import jax.numpy as jnp
from jax import lax
from jax.experimental import pallas as pl
from jax.experimental.pallas import tpu as pltpu
from jax.sharding import PartitionSpec as P

PAIRS, QLEN, DLEN, DPAD, HID, DIM = 8, 32, 300, 304, 768, 128
CHIPS, CORES, DEVICES = 64, 2, 128
LANES = PAIRS * QLEN
GROUPS, PER_GROUP = 8, 8


def hops(offset):
    return (0, 1, 2, 1)[offset]


def plan():
    tiles = [(dx, k1, k2) for dx in range(4) for k1 in range(4) for k2 in range(4)]
    gen = lambda t: (t[0] != 0) + hops(t[1]) + hops(t[2])
    dist = lambda t: sum(hops(o) for o in t)
    order = sorted(tiles, key=lambda t: (gen(t), dist(t), t))
    first, rest = order[:8], order[8:]
    waits = [[], rest[:16]] + [rest[16 + 8 * n:24 + 8 * n] for n in range(5)] + [[]]
    near = [t for t in rest if gen(t) == 2 and dist(t) == 2][:8]
    middle = [t for t in rest if t not in near]
    groups = [first] + [middle[8 * n:8 * n + 8] for n in range(6)] + [near]
    return first, waits, groups


def step_of(dx, axis, amount):
    along_y = (dx % 2 == 0) == (axis == 0)
    return (amount, 0) if along_y else (0, amount)


def forwards(tile):
    dx, k1, k2 = tile
    even = dx < 2
    go, back = (3, 1) if even else (1, -1)
    out = []
    if k1 == 0 and k2 == 0:
        out += [step_of(dx, 0, 1), step_of(dx, 0, -1)]
    if k2 == 0:
        out += [step_of(dx, 1, 1), step_of(dx, 1, -1)]
        if k1 == go:
            out.append(step_of(dx, 0, back))
    elif k2 == go:
        out.append(step_of(dx, 1, back))
    return out


def unit_rows(product):
    return product * lax.rsqrt(jnp.sum(product * product, axis=-1, keepdims=True))


def fold_lanes(row, shifts, combine):
    for shift in shifts:
        row = combine(row, pltpu.roll(row, shift, axis=1))
    return row


def kernel(qh_hbm, dh_hbm, nh_hbm, w_ref, qmask_ref, dmask_ref, nmask_ref, teacher_ref, tau_ref,
           loss_ref, mean_ref,
           qh, hidden, tiles, docs, negs, lens, hard, res_out, res_in, sum_out, sum_in,
           load_sem, q_sem, tile_send, tile_recv, doc_send, doc_recv, res_send, res_recv, sum_send, sum_recv):
    first, waits, groups = plan()
    me = lax.axis_index('data')
    core, chip = lax.rem(me, 2), lax.div(me, 2)
    cx, cy, cz = lax.rem(chip, 4), lax.rem(lax.div(chip, 4), 4), lax.div(chip, 16)
    wrap = lambda v: lax.rem(v + 8, 4)

    def chip_at(dx, dy, dz):
        return wrap(cz + dz) * 16 + wrap(cy + dy) * 4 + wrap(cx + dx)

    def target(dx, dy, dz):
        return {'data': chip_at(dx, dy, dz) * 2 + core}

    def slot_of(tile):
        dx, k1, k2 = tile
        return chip_at(dx, k1, k2) if dx % 2 == 0 else chip_at(dx, k2, k1)

    def tile_copy(slot, device):
        return pltpu.make_async_remote_copy(
            src_ref=tiles.at[slot], dst_ref=tiles.at[slot], send_sem=tile_send, recv_sem=tile_recv.at[slot],
            device_id=device, device_id_type=pl.DeviceIdType.MESH)

    def await_tile(tile):
        tile_copy(slot_of(tile), target(1, 0, 0)).wait_recv()

    def pass_on(tile):
        for dy, dz in forwards(tile):
            tile_copy(slot_of(tile), target(0, dy, dz)).start()

    load_q = pltpu.make_async_copy(qh_hbm, qh, q_sem)
    load_q.start()
    load_docs = [pltpu.make_async_copy(dh_hbm.at[j], hidden.at[j], load_sem.at[j]) for j in range(8)]
    load_negs = [pltpu.make_async_copy(nh_hbm.at[j // 2, j % 2], hidden.at[8 + j], load_sem.at[8 + j])
                 for j in range(16)]
    for copy in load_docs + load_negs:
        copy.start()

    barrier = pltpu.get_barrier_semaphore()
    for move in ((1, 0, 0), (2, 0, 0), (3, 0, 0), (0, 1, 0), (0, 3, 0), (0, 0, 1), (0, 0, 3)):
        pl.semaphore_signal(barrier, inc=1, device_id=target(*move), device_id_type=pl.DeviceIdType.MESH)
    pl.semaphore_signal(barrier, inc=1, device_id={'data': chip * 2 + 1 - core}, device_id_type=pl.DeviceIdType.MESH)

    w = w_ref[...]
    lane = lax.broadcasted_iota(jnp.int32, (1, LANES), 1)

    load_q.wait()
    q_unit = unit_rows(jnp.dot(qh[...].reshape(LANES, HID), w, preferred_element_type=jnp.float32)).astype(jnp.bfloat16)
    row_id = lax.broadcasted_iota(jnp.int32, (LANES, LANES), 0)
    col_id = lax.broadcasted_iota(jnp.int32, (LANES, LANES), 1)
    shuffle = (row_id == (col_id & 7) * QLEN + (col_id >> 3)).astype(jnp.float32).astype(jnp.bfloat16)
    q_cols = lax.dot_general(q_unit, shuffle, (((0,), (0,)), ((), ())), preferred_element_type=jnp.float32)
    q_len = jnp.sum(qmask_ref[...].astype(jnp.float32), axis=1, keepdims=True)
    sub8 = lax.broadcasted_iota(jnp.int32, (PAIRS, LANES), 0)
    lane8 = lax.broadcasted_iota(jnp.int32, (PAIRS, LANES), 1)
    q_live = jnp.where(((lane8 >> 3).astype(jnp.float32) < q_len) & ((lane8 & 7) == sub8), 1.0, 0.0)
    q_live = jnp.sum(q_live, axis=0, keepdims=True)
    tiles[chip] = jnp.where(q_live > 0, q_cols, 0.0).astype(jnp.bfloat16)

    d_len = jnp.sum(dmask_ref[...], axis=1, keepdims=True)
    lens[pl.ds(0, 8)] = jnp.broadcast_to(d_len, (8, 128))
    n_len = jnp.sum(nmask_ref[...], axis=2, keepdims=True)
    for j in range(16):
        lens[pl.ds(8 + j, 1)] = jnp.broadcast_to(n_len[j // 2, j % 2:j % 2 + 1], (1, 128))

    pl.semaphore_wait(barrier, 8)
    for dx in (1, 3, 2):
        tile_copy(chip, target(dx, 0, 0)).start()
    pass_on((0, 0, 0))

    row304 = lax.broadcasted_iota(jnp.int32, (DPAD, DIM), 0)

    def project(j):
        unit = unit_rows(jnp.dot(hidden[j], w, preferred_element_type=jnp.float32))
        unit = jnp.concatenate([unit, unit[:DPAD - DLEN]], axis=0)
        return jnp.where(row304 < lens[pl.ds(j, 1)], unit, unit[0:1]).astype(jnp.bfloat16)

    for copy in load_docs:
        copy.wait()
    for j in range(8):
        docs[core, j] = project(j)

    for copy in load_negs:
        copy.wait()
    doc_copy = pltpu.make_async_remote_copy(
        src_ref=docs.at[core], dst_ref=docs.at[core], send_sem=doc_send, recv_sem=doc_recv,
        device_id={'data': chip * 2 + 1 - core}, device_id_type=pl.DeviceIdType.MESH)
    doc_copy.start()

    def neg_body(n, carry):
        for u in range(8):
            negs[n * 8 + u] = project(8 + n * 8 + u)
        return carry

    lax.fori_loop(0, 2, neg_body, 0)

    for tile in first[1:]:
        await_tile(tile)
        pass_on(tile)

    def best(doc_at, cols):
        rows = []
        for j in range(16):
            sim = jnp.dot(doc_at(j), cols, preferred_element_type=jnp.float32)
            rows.append(jnp.max(sim, axis=0, keepdims=True))
        best_rows = jnp.concatenate(rows, axis=0)
        return fold_lanes(best_rows[:, :128] + best_rows[:, 128:], (8, 16, 32, 64), jnp.add)

    hard[...] = best(lambda j: negs[j], tiles[chip])
    doc_copy.wait_recv()

    sub16 = lax.broadcasted_iota(jnp.int32, (16, 128), 0)
    lane16 = lax.broadcasted_iota(jnp.int32, (16, 128), 1)
    keep = (lane16 >> 3) == sub16

    def score(slot):
        block = best(lambda j: docs[j // 8, j % 8], tiles[slot])
        res_out[slot] = jnp.sum(jnp.where(keep, block, 0.0), axis=0, keepdims=True)

    def slot_in_group(g, u):
        codes = []
        for tile in (group[u] for group in groups):
            dx, k1, k2 = tile
            dy, dz = (k1, k2) if dx % 2 == 0 else (k2, k1)
            codes.append(dz * 16 + dy * 4 + dx)
        code = codes[0]
        for n in range(1, GROUPS):
            code = jnp.where(g == n, codes[n], code)
        return chip_at(lax.rem(code, 4), lax.rem(lax.div(code, 4), 4), lax.div(code, 16))

    def res_copy(slot):
        return pltpu.make_async_remote_copy(
            src_ref=res_out.at[slot], dst_ref=res_in.at[chip], send_sem=res_send, recv_sem=res_recv,
            device_id={'data': slot * 2 + core}, device_id_type=pl.DeviceIdType.MESH)

    def send_results(g):
        for u in range(PER_GROUP):
            slot = slot_in_group(g, u)

            @pl.when(slot != chip)
            def _():
                res_copy(slot).start()

    def group_body(g, carry):
        for n in range(1, GROUPS):
            if waits[n]:
                @pl.when(g == n)
                def _(n=n):
                    for tile in waits[n]:
                        await_tile(tile)
                        pass_on(tile)

        @pl.when(g > 0)
        def _():
            send_results(g - 1)

        for u in range(PER_GROUP):
            score(slot_in_group(g, u))
        return carry

    lax.fori_loop(0, GROUPS, group_body, 0)
    send_results(GROUPS - 1)

    tau = tau_ref[0, 0]
    fold8 = (8, 16, 32, 64)
    sub = lax.broadcasted_iota(jnp.int32, (8, 128), 0)
    col = lax.broadcasted_iota(jnp.int32, (8, 128), 1)
    row_lane = lax.broadcasted_iota(jnp.int32, (1, 128), 1)
    own = res_out[chip]
    res_in[chip] = own
    pos = fold_lanes(jnp.where((row_lane >> 3) == core * 8 + (row_lane & 7), own, 0.0), fold8, jnp.add) / tau
    hard_all = hard[...]
    student = [pos] + [jnp.sum(jnp.where(sub16 == 2 * (lane16 & 7) + k, hard_all, 0.0), axis=0, keepdims=True) / tau
                       for k in range(2)]
    teacher = [jnp.sum(jnp.where((col & 7) == sub, jnp.broadcast_to(teacher_ref[:, k:k + 1], (8, 128)), 0.0),
                       axis=0, keepdims=True) for k in range(3)]

    def log_softmax(rows):
        top = jnp.maximum(jnp.maximum(rows[0], rows[1]), rows[2])
        total = jnp.exp(rows[0] - top) + jnp.exp(rows[1] - top) + jnp.exp(rows[2] - top)
        return [row - top - jnp.log(total) for row in rows]

    student_log, teacher_log = log_softmax(student), log_softmax(teacher)
    kl = sum(jnp.exp(t) * (t - s) for s, t in zip(student_log, teacher_log))

    pltpu.make_async_remote_copy(
        src_ref=res_out.at[pl.ds(0, CHIPS - 1)], dst_ref=res_in.at[pl.ds(0, CHIPS - 1)], send_sem=res_send,
        recv_sem=res_recv, device_id=target(1, 0, 0), device_id_type=pl.DeviceIdType.MESH).wait_recv()
    logits = res_in[...] / tau
    top = fold_lanes(jnp.max(logits, axis=0), fold8, jnp.maximum)
    total = fold_lanes(jnp.sum(jnp.exp(logits - top), axis=0), fold8, jnp.add)
    loss = top + jnp.log(total) - pos + kl
    loss_ref[...] = loss[:, :PAIRS]

    part = fold_lanes(loss, (1, 2, 4), jnp.add)
    sum_out[...] = part
    sum_in[me] = part

    def sum_copy(n):
        return pltpu.make_async_remote_copy(
            src_ref=sum_out, dst_ref=sum_in.at[me], send_sem=sum_send, recv_sem=sum_recv,
            device_id={'data': lax.rem(me + n, DEVICES)}, device_id_type=pl.DeviceIdType.MESH)

    def send_sum(n, carry):
        sum_copy(n).start()
        return carry

    lax.fori_loop(1, DEVICES, send_sum, 0)

    doc_copy.wait_send()
    pltpu.make_async_remote_copy(
        src_ref=tiles.at[pl.ds(0, CHIPS - 1)], dst_ref=tiles.at[pl.ds(0, CHIPS - 1)], send_sem=tile_send,
        recv_sem=tile_recv.at[0], device_id=target(1, 0, 0), device_id_type=pl.DeviceIdType.MESH).wait_send()
    pltpu.make_async_remote_copy(
        src_ref=res_out.at[pl.ds(0, CHIPS - 1)], dst_ref=res_in.at[pl.ds(0, CHIPS - 1)], send_sem=res_send,
        recv_sem=res_recv, device_id=target(1, 0, 0), device_id_type=pl.DeviceIdType.MESH).wait_send()
    all_sums = pltpu.make_async_remote_copy(
        src_ref=sum_in.at[pl.ds(0, DEVICES - 1)], dst_ref=sum_in.at[pl.ds(0, DEVICES - 1)], send_sem=sum_send,
        recv_sem=sum_recv, device_id=target(1, 0, 0), device_id_type=pl.DeviceIdType.MESH)
    all_sums.wait_recv()
    mean_ref[...] = (jnp.sum(sum_in[...], axis=0) / (PAIRS * DEVICES))[:, :1]
    all_sums.wait_send()


def solution(mesh):
    batch = ('replica', 'data')

    def local_loss(query_hidden, doc_hidden, neg_hidden, query_mask, doc_mask, neg_mask, teacher, w_proj, temperature):
        vmem, anyspace = pl.BlockSpec(memory_space=pltpu.VMEM), pl.BlockSpec(memory_space=pl.ANY)
        dma = pltpu.SemaphoreType.DMA
        loss, mean = pl.pallas_call(
            kernel,
            name='late_interaction',
            out_shape=(jax.ShapeDtypeStruct((1, PAIRS), jnp.float32), jax.ShapeDtypeStruct((1, 1), jnp.float32)),
            in_specs=[anyspace] * 3 + [vmem] * 5 + [pl.BlockSpec(memory_space=pltpu.SMEM)],
            out_specs=(vmem, vmem),
            scratch_shapes=[
                pltpu.VMEM((PAIRS, QLEN, HID), jnp.bfloat16),
                pltpu.VMEM((24, DLEN, HID), jnp.bfloat16),
                pltpu.VMEM((CHIPS, DIM, LANES), jnp.bfloat16),
                pltpu.VMEM((CORES, 8, DPAD, DIM), jnp.bfloat16),
                pltpu.VMEM((16, DPAD, DIM), jnp.bfloat16),
                pltpu.VMEM((24, 128), jnp.int32),
                pltpu.VMEM((16, 128), jnp.float32),
                pltpu.VMEM((CHIPS, 1, 128), jnp.float32),
                pltpu.VMEM((CHIPS, 1, 128), jnp.float32),
                pltpu.VMEM((1, 128), jnp.float32),
                pltpu.VMEM((DEVICES, 1, 128), jnp.float32),
                dma((24,)), dma, dma, dma((CHIPS,)), dma, dma, dma, dma, dma, dma,
            ],
            compiler_params=pltpu.CompilerParams(
                collective_id=0, has_side_effects=True, vmem_limit_bytes=60 * 2**20),
        )(query_hidden, doc_hidden, neg_hidden, w_proj, query_mask, doc_mask, neg_mask, teacher,
          temperature.reshape(1, 1))
        return loss.reshape(PAIRS), mean.reshape(1)

    in_specs = (P(batch, None, None), P(batch, None, None), P(batch, None, None, None), P(batch, None), P(batch, None),
                P(batch, None, None), P(batch, None), P(None, None), P())
    return jax.shard_map(local_loss, mesh=mesh, in_specs=in_specs, out_specs=(P(batch), P('replica')), check_vma=False)
```
